128 devices in a mesh: days: 32 (over z, y, core), cols: 4 (over x).
Axes of the slice: x: 4, y: 4, z: 4, core: 2. Of those that a mesh axis runs over, the one named last changes fastest.
Arguments:
- stations: int32 [256, 8], replicated, may hold values from 0 to 127, as said below
- counts: int32 [256], replicated, may hold values from 4 to 8, as said below
- q_cols: bfloat16 [16384, 16384], P(None, ('days', 'cols')), may hold values from -6 to 6, as said below
- glob_solution: float32 [16384], P(('days', 'cols')), may hold values from -6 to 6
- inv_blocks: bfloat16 [256, 4096, 128], P('days', 'cols')
- coupling: bfloat16 [256, 4096, 1024], P('days', 'cols'), may hold values from -0.1875 to 0.1875
- local_rhs: float32 [256, 4096], P('days', 'cols'), may hold values from -6 to 6
Outputs:
- local_solution: float32 [256, 4096], P('days', 'cols')
- cov_diag: float32 [256, 4096], P('days', 'cols')
The draws below stay inside these ranges and needn't reach their ends.
Inputs may be any that keep to these rules, and one draw needn't show every extreme that they name: `stations`: each day names 8 different blocks, the first counts of them observed; the days of one index of days name one block at most 1 times, and some observed block exactly 1 times. `counts`: the first day of every index of days observes 8 blocks. q_cols equals its transpose exactly.
All inputs are finite; a program needn't handle non-finite values.
Results may differ from the reference program's by a relative error of at most 0.0035.
Values may be sent and summed in bfloat16 or wider, within the bound.
No kernel may reach another device: no remote copies, remote signals or barrier semaphores. Data moves between devices by JAX's collectives and lax.ppermute only.
A program may use at most 192 MiB of HBM per device.

```python
import jax
import jax.numpy as jnp
from jax import lax

BW = 128
KMAX = 8
L = 4096
DAY_DEV = 8
NB = 128
GP = 16384
DAYS = 256
M = 1024


def draw_stations(key, part):
    shards = DAYS // DAY_DEV
    keys = jax.random.split(key, shards)
    perms = jax.vmap(lambda single: jax.random.permutation(single, NB))(keys)
    positions = jnp.arange(DAY_DEV * KMAX) % NB
    return perms[:, positions].reshape(DAYS, KMAX).astype(jnp.int32)


def draw_counts(key, part):
    drawn = jax.random.randint(key, (DAYS,), KMAX // 2, KMAX + 1)
    first = jnp.arange(DAYS) % DAY_DEV == 0
    return jnp.where(first, KMAX, drawn).astype(jnp.int32)


def draw_q_cols(key, part):
    rows_i = jnp.arange(GP)[:, None]
    cols_j = jnp.arange(GP)[None, :]
    upper = rows_i <= cols_j
    noise = jnp.clip(jax.random.normal(jax.random.fold_in(key, 23), (GP, GP), jnp.float32), -6.0, 6.0)
    return jnp.where(upper, noise, noise.T).astype(jnp.bfloat16)


def draw_inv_blocks(key, part):
    groups = L // BW
    noise = jax.random.normal(jax.random.fold_in(key, 11), (DAYS, groups, BW, BW), jnp.float32) * (0.5 / BW ** 0.5)
    sym = 0.5 * (noise + jnp.swapaxes(noise, 2, 3))
    diag = jax.random.uniform(jax.random.fold_in(key, 12), (DAYS, groups, BW), jnp.float32, 1.0, 2.0)
    eye = jnp.eye(BW, dtype=jnp.float32)
    blocks = sym + diag[..., :, None] * eye
    return blocks.reshape(DAYS, L, BW).astype(jnp.bfloat16)


def steps_of(stream_key, dims, cuts, low, top_value):
    level = 1.0
    for position, blocks in cuts:
        draws = jax.random.uniform(jax.random.fold_in(jax.random.fold_in(stream_key, 6), position), (blocks,), jnp.float32, low / len(cuts), top_value / len(cuts))
        level = level * jnp.repeat(jnp.exp(draws), dims[position] // blocks).reshape((-1,) + (1,) * (len(dims) - 1 - position))
    return level


def normal_values(stream_key, dims, width, bound, cuts=(), kind=jnp.bfloat16):
    result = jax.random.normal(stream_key, dims, jnp.float32) * width
    if len(cuts) > 0:
        result = steps_of(stream_key, dims, cuts, -0.22, 0.18) * result
    return jnp.clip(result, min=-bound, max=bound).astype(kind)


def setup_inputs(seed: int = 0) -> dict:
    seeds = jax.random.split(jax.random.key(seed), 8)
    return {
        "stations": draw_stations(jax.random.fold_in(seeds[7], 71), 0),
        "counts": draw_counts(jax.random.fold_in(seeds[7], 71), 0),
        "q_cols": draw_q_cols(jax.random.fold_in(seeds[7], 71), 0),
        "glob_solution": normal_values(seeds[3], (GP,), 1.0, 6.0, ((0, 128),), jnp.float32),
        "inv_blocks": draw_inv_blocks(jax.random.fold_in(seeds[7], 71), 0),
        "coupling": normal_values(seeds[5], (DAYS, L, M), M ** -0.5, 0.1875, ((0, 32), (1, 4))),
        "local_rhs": normal_values(seeds[6], (DAYS, L), 1.0, 6.0, ((0, 32), (1, 4)), jnp.float32),
    }


def one_day(q_cols, glob_solution, inputs):
    station_row, count, inv_day, coup_day, rhs_day = inputs
    groups = L // BW
    valid = (jnp.arange(KMAX) < count).astype(jnp.float32)
    colmask = jnp.repeat(valid, BW)
    index = (station_row[:, None] * BW + jnp.arange(BW)[None, :]).reshape(M).astype(jnp.int32)
    x_sel = (glob_solution[index] * colmask).astype(jnp.bfloat16)
    resid = (rhs_day - jnp.dot(coup_day, x_sel, preferred_element_type=jnp.float32)).astype(jnp.bfloat16)
    inv_g = inv_day.reshape(groups, BW, BW).astype(jnp.float32)
    solved = jnp.einsum('gij,gj->gi', inv_g, resid.reshape(groups, BW).astype(jnp.float32)).reshape(L)
    gfull = jnp.einsum('gij,gjm->gim', inv_g, coup_day.reshape(groups, BW, M).astype(jnp.float32)).reshape(L, M)
    gmat = (gfull * colmask[None, :]).astype(jnp.bfloat16)
    qrows = jnp.take(q_cols, index, axis=0)
    qsub = jnp.take(qrows, index, axis=1)
    hmat = jnp.dot(gmat, qsub, preferred_element_type=jnp.float32)
    diag_inv = jnp.diagonal(inv_g, axis1=1, axis2=2).reshape(L)
    cov = diag_inv + jnp.sum(hmat * gmat.astype(jnp.float32), axis=1)
    return solved, cov


def reference(stations, counts, q_cols, glob_solution, inv_blocks, coupling, local_rhs):
    solved, cov = lax.map(lambda inputs: one_day(q_cols, glob_solution, inputs),
                          (stations, counts, inv_blocks, coupling, local_rhs))
    return solved, cov
```

```python
import functools

import jax
import jax.numpy as jnp
from jax import lax
from jax.experimental import pallas as pl
from jax.experimental.pallas import tpu as pltpu
from jax.sharding import PartitionSpec as P

BW = 128
KMAX = 8
QROWS = 144
CHUNKS = (3, 3, 2)


def pack_kernel(shards, day_dev, pos_ref, st_ref, q_ref, glob_ref, out_ref, blocks, items, in_sem, out_sem):
    slots = day_dev * KMAX

    def copies(shard):
        pos = pos_ref[shard]
        day = pos // KMAX
        slot = pos % KMAX
        made = []
        for off in range(5):
            other = st_ref[shard * slots + day * KMAX + (slot + off) % KMAX]
            rows = pl.ds(pl.multiple_of(other * BW, BW), BW)
            made.append(
                pltpu.make_async_copy(q_ref.at[rows, :], blocks.at[shard, off], in_sem.at[shard, off])
            )
        return made

    def out_copy(shard):
        return pltpu.make_async_copy(items.at[shard], out_ref.at[shard], out_sem.at[shard])

    @pl.loop(0, shards)
    def _(shard):
        @pl.when(pos_ref[shard] >= 0)
        def _():
            for copy in copies(shard):
                copy.start()

    x_rows = jnp.broadcast_to(glob_ref[...], (8, BW))

    @pl.loop(0, shards)
    def _(shard):
        @pl.when(pos_ref[shard] >= 0)
        def _():
            for copy in copies(shard):
                copy.wait()
            upper = (pos_ref[shard] % KMAX) < KMAX // 2
            half = blocks[shard, 4]
            lane = lax.broadcasted_iota(jnp.int32, (64, BW), 1)
            rolled = pltpu.roll(half[:64].astype(jnp.float32), 64, 1).astype(jnp.bfloat16)
            packed = jnp.where(lane < 64, rolled, half[64:])
            half = jnp.where(upper, half[:64], packed)
            diag = blocks[shard, 0]
            lane32 = lax.broadcasted_iota(jnp.int32, (32, BW), 1)
            corner = jnp.where(
                lane32 < 64,
                pltpu.roll(diag[64:96].astype(jnp.float32), 64, 1),
                diag[96:].astype(jnp.float32),
            )
            for q in range(4):
                for off in range(1, 4):
                    items[shard, q, 32 * (off - 1) : 32 * off, :] = blocks[shard, off, 32 * q : 32 * (q + 1), :]
                items[shard, q, 96:112, :] = half[16 * q : 16 * (q + 1)]
                items[shard, q, 112:128, :] = diag[16 * q : 16 * (q + 1)]
                items[shard, q, 128:144, :] = jnp.concatenate(
                    [corner[8 * q : 8 * (q + 1)], x_rows], axis=0
                ).astype(jnp.bfloat16)
            out_copy(shard).start()

    @pl.loop(0, shards)
    def _(shard):
        @pl.when(pos_ref[shard] >= 0)
        def _():
            out_copy(shard).wait()


def pack_items(pos, st_flat, q_cols, glob_row, shards, day_dev):
    return pl.pallas_call(
        functools.partial(pack_kernel, shards, day_dev),
        out_shape=jax.ShapeDtypeStruct((shards, 4, QROWS, BW), jnp.bfloat16),
        grid_spec=pltpu.PrefetchScalarGridSpec(
            num_scalar_prefetch=2,
            grid=(1,),
            in_specs=[
                pl.BlockSpec(memory_space=pl.ANY),
                pl.BlockSpec((1, BW), lambda i, *_: (0, 0)),
            ],
            out_specs=pl.BlockSpec(memory_space=pl.ANY),
            scratch_shapes=[
                pltpu.VMEM((shards, 5, BW, BW), jnp.bfloat16),
                pltpu.VMEM((shards, 4, QROWS, BW), jnp.bfloat16),
                pltpu.SemaphoreType.DMA((shards, 5)),
                pltpu.SemaphoreType.DMA((shards,)),
            ],
        ),
        cost_estimate=pl.CostEstimate(flops=10_000_000, bytes_accessed=10_000_000, transcendentals=0),
        name="pack_items",
    )(pos, st_flat, q_cols, glob_row)


def gmat_kernel(cnt_ref, inv_ref, coup_ref, rhs_ref, x_ref, g_ref, sol_ref, dinv_ref):
    count = cnt_ref[pl.program_id(0)]
    rows, span = coup_ref.shape[1:]
    groups = rows // BW
    x8 = jnp.concatenate([x_ref[0, k, 8:9, :].astype(jnp.float32) for k in range(KMAX)], axis=0)
    keep = lax.broadcasted_iota(jnp.int32, (KMAX, BW), 0) < count
    x_t = jnp.where(keep, x8, 0.0).T
    rhs_t = rhs_ref[0].T
    x_col = jnp.concatenate(
        [jnp.broadcast_to(x_t[:, k : k + 1], (BW, BW)) for k in range(KMAX)], axis=0
    ).astype(jnp.bfloat16)
    lane = lax.broadcasted_iota(jnp.int32, (BW, BW), 1)
    row = lax.broadcasted_iota(jnp.int32, (BW, BW), 0)
    mask = (lax.broadcasted_iota(jnp.int32, (1, span), 1) // BW) < count
    solved = jnp.zeros((BW, BW), jnp.float32)
    for g in range(groups):
        part = slice(g * BW, (g + 1) * BW)
        inv_g = inv_ref[0, part, :]
        coup_g = coup_ref[0, part, :]
        dots = jnp.dot(coup_g, x_col, preferred_element_type=jnp.float32)
        resid = (rhs_t[:, g : g + 1] - dots).astype(jnp.bfloat16)
        resid = jnp.where(lane == g, resid, jnp.zeros_like(resid))
        solved += jnp.dot(inv_g, resid, preferred_element_type=jnp.float32)
        full = jnp.dot(inv_g, coup_g, preferred_element_type=jnp.float32)
        g_ref[0, part, :] = jnp.where(mask, full, 0.0).astype(jnp.bfloat16)
        inv_f = inv_g.astype(jnp.float32)
        dinv_ref[0, g : g + 1, :] = jnp.sum(jnp.where(lane == row, inv_f, 0.0), axis=0, keepdims=True)
    sol_ref[0] = solved.T[:groups]


def gmat_call(counts, inv_blocks, coupling, rhs, shard):
    days, rows, span = coupling.shape
    groups = rows // BW
    return pl.pallas_call(
        gmat_kernel,
        out_shape=(
            jax.ShapeDtypeStruct((days, rows, span), jnp.bfloat16),
            jax.ShapeDtypeStruct((days, groups, BW), jnp.float32),
            jax.ShapeDtypeStruct((days, groups, BW), jnp.float32),
        ),
        grid_spec=pltpu.PrefetchScalarGridSpec(
            num_scalar_prefetch=1,
            grid=(days,),
            in_specs=[
                pl.BlockSpec((1, rows, BW), lambda i, *_: (i, 0, 0)),
                pl.BlockSpec((1, rows, span), lambda i, *_: (i, 0, 0)),
                pl.BlockSpec((1, groups, BW), lambda i, *_: (i, 0, 0)),
                pl.BlockSpec((1, KMAX, 16, BW), lambda i, *_: (i, 0, 0, 0)),
            ],
            out_specs=[
                pl.BlockSpec((1, rows, span), lambda i, *_: (i, 0, 0)),
                pl.BlockSpec((1, groups, BW), lambda i, *_: (i, 0, 0)),
                pl.BlockSpec((1, groups, BW), lambda i, *_: (i, 0, 0)),
            ],
        ),
        cost_estimate=pl.CostEstimate(
            flops=2 * days * rows * span * 2 * BW, bytes_accessed=days * rows * span * 4, transcendentals=0
        ),
        name="gmat",
    )(counts, inv_blocks, coupling, rhs, shard)


def cov_kernel(days, me_ref, g_ref, dinv_ref, own_ref, prev_ref, next_ref, far_a_ref, far_b_ref, out_ref, items, weights, sems):
    step = pl.program_id(0)
    me = me_ref[0]
    slots = days * KMAX
    half = slots // 2
    rows, span = g_ref.shape[1:]
    groups = rows // BW
    quad = KMAX // 2

    def copies(day, slot):
        made = []
        for n, (ref, away) in enumerate(((own_ref, 0), (prev_ref, 3), (next_ref, 1))):
            made.append(
                pltpu.make_async_copy(
                    ref.at[pl.ds(day * KMAX, KMAX)], items.at[slot, lax.rem(me + away, 4)], sems.at[slot, n]
                )
            )
        return made

    def far_copy(ref, start, part, slot):
        dst = items.at[slot, lax.rem(me + 2, 4), pl.ds(part * quad, quad)]
        return pltpu.make_async_copy(ref.at[pl.ds(start, quad)], dst, sems.at[slot, 3 + part])

    def start(day, slot):
        for copy in copies(day, slot):
            copy.start()
        for part in range(2):
            first = day * KMAX + part * quad

            @pl.when(first < half)
            def _():
                far_copy(far_a_ref, first, part, slot).start()

            @pl.when(first >= half)
            def _():
                far_copy(far_b_ref, first - half, part, slot).start()

    @pl.when(step == 0)
    def _():
        weights[...] = jnp.zeros_like(weights)
        start(0, 0)

    slot = lax.rem(step, 2)
    for copy in copies(step, slot):
        copy.wait()
    for part in range(2):
        far_copy(far_a_ref, 0, part, slot).wait()

    @pl.when(step + 1 < days)
    def _():
        start(step + 1, 1 - slot)

    for k in range(KMAX):
        j, e = k // 2, k % 2
        lanes = slice(e * BW, (e + 1) * BW)
        lane64 = lax.broadcasted_iota(jnp.int32, (64, BW), 1)
        lane32 = lax.broadcasted_iota(jnp.int32, (32, BW), 1)
        for off in range(1, 4):
            base = (e + off) * BW
            for q in range(4):
                weights[j, base + 32 * q : base + 32 * (q + 1), lanes] = items[slot, q, k, 32 * (off - 1) : 32 * off, :]
        far = jnp.concatenate([items[slot, q, k, 96:112, :] for q in range(4)], axis=0)
        base = (e + 4) * BW
        if k < quad:
            weights[j, base : base + 64, lanes] = far
        else:
            far_f = far.astype(jnp.float32)
            weights[j, base : base + 64, lanes] = jnp.where(lane64 >= 64, pltpu.roll(far_f, 64, 1), 0.0).astype(jnp.bfloat16)
            weights[j, base + 64 : base + 128, lanes] = jnp.where(lane64 >= 64, far_f, 0.0).astype(jnp.bfloat16)
        top = jnp.concatenate([items[slot, q, k, 112:128, :] for q in range(4)], axis=0).astype(jnp.float32)
        corner = jnp.concatenate(
            [items[slot, q, k, 128:144, :].astype(jnp.float32)[:8] for q in range(4)], axis=0
        )
        base = e * BW
        weights[j, base : base + 64, lanes] = jnp.where(lane64 < 64, 0.5 * top, top).astype(jnp.bfloat16)
        low = jnp.concatenate([pltpu.roll(corner, 64, 1), corner], axis=0)
        weights[j, base + 64 : base + 128, lanes] = jnp.where(lane64 >= 64, 0.5 * low, 0.0).astype(jnp.bfloat16)

    block = 256
    for r in range(rows // block):
        here = slice(r * block, (r + 1) * block)
        acc = jnp.zeros((block, BW), jnp.float32)
        for j in range(quad):
            left = jnp.concatenate(
                [g_ref[0, here, ((j + s) % quad) * 2 * BW : ((j + s) % quad + 1) * 2 * BW] for s in range(3)], axis=1
            )
            h = jnp.dot(left, weights[j], preferred_element_type=jnp.float32)
            g_f = g_ref[0, here, j * 2 * BW : (j + 1) * 2 * BW].astype(jnp.float32)
            prod = h * g_f
            acc += prod[:, :BW] + prod[:, BW:]
        for b in range(block // BW):
            g = r * (block // BW) + b
            total = jnp.sum(acc[b * BW : (b + 1) * BW].T, axis=0, keepdims=True)
            out_ref[0, g : g + 1, :] = dinv_ref[0, g : g + 1, :] + 2.0 * total


def cov_call(me, gmat, dinv, own, prev, nxt, far_a, far_b, first, days):
    rows, span = gmat.shape[1:]
    groups = rows // BW
    any_spec = pl.BlockSpec(memory_space=pl.ANY)
    return pl.pallas_call(
        functools.partial(cov_kernel, days),
        out_shape=jax.ShapeDtypeStruct((days, groups, BW), jnp.float32),
        grid_spec=pltpu.PrefetchScalarGridSpec(
            num_scalar_prefetch=1,
            grid=(days,),
            in_specs=[
                pl.BlockSpec((1, rows, span), lambda i, *_: (i + first, 0, 0)),
                pl.BlockSpec((1, groups, BW), lambda i, *_: (i + first, 0, 0)),
                any_spec,
                any_spec,
                any_spec,
                any_spec,
                any_spec,
            ],
            out_specs=pl.BlockSpec((1, groups, BW), lambda i, *_: (i, 0, 0)),
            scratch_shapes=[
                pltpu.VMEM((2, 4, KMAX, QROWS, BW), jnp.bfloat16),
                pltpu.VMEM((KMAX // 2, 6 * BW, 2 * BW), jnp.bfloat16),
                pltpu.SemaphoreType.DMA((2, 5)),
            ],
        ),
        cost_estimate=pl.CostEstimate(
            flops=2 * days * rows * span * 768, bytes_accessed=days * (rows * span * 2 + 1_200_000), transcendentals=0
        ),
        name=f"cov_{first}",
    )(me, gmat, dinv, own, prev, nxt, far_a, far_b)


def local(stations, counts, q_cols, glob_solution, inv_blocks, coupling, local_rhs):
    shards = lax.axis_size("days")
    ncols = lax.axis_size("cols")
    me = lax.axis_index("cols")
    my_shard = lax.axis_index("days")
    owner = my_shard * ncols + me
    day_dev, rows, width = inv_blocks.shape
    slots = day_dev * KMAX
    groups = rows // BW

    shard_st = stations.reshape(shards, slots)
    order = jnp.arange(slots, dtype=jnp.int32)
    pos = jnp.max(jnp.where(shard_st == owner, order[None, :], -1), axis=1)
    items = pack_items(pos, stations.reshape(-1), q_cols, glob_solution.reshape(1, BW), shards, day_dev)
    got = lax.all_to_all(
        items.reshape(shards * ncols, QROWS, BW), ("days", "cols"), split_axis=0, concat_axis=0, tiled=True
    )
    my_st = lax.dynamic_slice_in_dim(stations, my_shard * day_dev, day_dev, 0).reshape(slots)
    my_counts = lax.dynamic_slice_in_dim(counts, my_shard * day_dev, day_dev, 0)
    ahead = [(i, (i + 1) % ncols) for i in range(ncols)]
    back = [(i, (i - 1) % ncols) for i in range(ncols)]

    owns, hops = [], []
    first = 0
    for days in CHUNKS:
        own = jnp.take(got, my_st[first * KMAX : (first + days) * KMAX], axis=0)
        prev = lax.ppermute(own, "cols", ahead)
        nxt = lax.ppermute(own, "cols", back)
        owns.append(own)
        hops.append((prev, nxt))
        first += days
    x_rows = jnp.take(got[:, QROWS - 16 :, :], my_st, axis=0).reshape(day_dev, KMAX, 16, BW)
    gmat, solved, dinv = gmat_call(
        my_counts, inv_blocks, coupling, local_rhs.reshape(day_dev, groups, BW), x_rows
    )
    covs = []
    first = 0
    for days, own, (prev, nxt) in zip(CHUNKS, owns, hops):
        half = days * KMAX // 2
        far_a = lax.ppermute(prev[:half], "cols", ahead)
        far_b = lax.ppermute(nxt[half:], "cols", back)
        covs.append(cov_call(me.reshape(1), gmat, dinv, own, prev, nxt, far_a, far_b, first, days))
        first += days
    cov = jnp.concatenate(covs, axis=0)
    return solved.reshape(day_dev, rows), cov.reshape(day_dev, rows)


def solution(mesh):
    return jax.shard_map(
        local,
        mesh=mesh,
        in_specs=(
            P(),
            P(),
            P(None, ("days", "cols")),
            P(("days", "cols")),
            P("days", "cols", None),
            P("days", "cols", None),
            P("days", "cols"),
        ),
        out_specs=(P("days", "cols"), P("days", "cols")),
        check_vma=False,
    )
```

```python
import functools

import jax
import jax.numpy as jnp
from jax import lax
from jax.experimental import pallas as pl
from jax.experimental.pallas import tpu as pltpu
from jax.sharding import PartitionSpec as P


BW = 128
KMAX = 8
QROWS = 112
OROWS = 112
CHUNKS = ((3, "ahead"), (3, "back"), (2, "direct"))


def pack_kernel(shards, day_dev, pos_ref, st_ref, q_ref, out_ref, blocks, items, in_sem, out_sem):
    slots = day_dev * KMAX

    def copies(shard):
        pos = pos_ref[shard]
        day = pos // KMAX
        slot = pos % KMAX
        made = []
        for n in range(4):
            other = st_ref[shard * slots + day * KMAX + (slot + n + 1) % KMAX]
            rows = pl.ds(pl.multiple_of(other * BW, BW), BW)
            made.append(pltpu.make_async_copy(q_ref.at[rows, :], blocks.at[shard, n], in_sem.at[shard, n]))
        return made

    def out_copy(shard):
        return pltpu.make_async_copy(items.at[shard], out_ref.at[shard], out_sem.at[shard])

    @pl.loop(0, shards)
    def _(shard):
        @pl.when(pos_ref[shard] >= 0)
        def _():
            for copy in copies(shard):
                copy.start()

    @pl.loop(0, shards)
    def _(shard):
        @pl.when(pos_ref[shard] >= 0)
        def _():
            for copy in copies(shard):
                copy.wait()
            upper = (pos_ref[shard] % KMAX) < KMAX // 2
            half = blocks[shard, 3]
            lane = lax.broadcasted_iota(jnp.int32, (64, BW), 1)
            turned = pltpu.roll(half[:64].astype(jnp.float32), 64, 1).astype(jnp.bfloat16)
            half = jnp.where(upper, half[:64], jnp.where(lane < 64, turned, half[64:]))
            for q in range(4):
                for n in range(3):
                    items[shard, q, 32 * n : 32 * (n + 1), :] = blocks[shard, n, 32 * q : 32 * (q + 1), :]
                items[shard, q, 96:112, :] = half[16 * q : 16 * (q + 1)]
            out_copy(shard).start()

    @pl.loop(0, shards)
    def _(shard):
        @pl.when(pos_ref[shard] >= 0)
        def _():
            out_copy(shard).wait()


def pack_items(pos, st_flat, q_cols, shards, day_dev):
    return pl.pallas_call(
        functools.partial(pack_kernel, shards, day_dev),
        out_shape=jax.ShapeDtypeStruct((shards, 4, QROWS, BW), jnp.bfloat16),
        grid_spec=pltpu.PrefetchScalarGridSpec(
            num_scalar_prefetch=2,
            grid=(1,),
            in_specs=[pl.BlockSpec(memory_space=pl.ANY)],
            out_specs=pl.BlockSpec(memory_space=pl.ANY),
            scratch_shapes=[
                pltpu.VMEM((shards, 4, BW, BW), jnp.bfloat16),
                pltpu.VMEM((shards, 4, QROWS, BW), jnp.bfloat16),
                pltpu.SemaphoreType.DMA((shards, 4)),
                pltpu.SemaphoreType.DMA((shards,)),
            ],
        ),
        cost_estimate=pl.CostEstimate(flops=5_000_000, bytes_accessed=8_000_000, transcendentals=0),
        name="pack",
    )(pos, st_flat, q_cols)


def own_kernel(me_ref, diag_ref, glob_ref, own_ref):
    diag = diag_ref[...]
    lane32 = lax.broadcasted_iota(jnp.int32, (32, BW), 1)
    rolled = pltpu.roll(diag[64:96].astype(jnp.float32), 64, 1).astype(jnp.bfloat16)
    own_ref[0:64, :] = diag[:64]
    own_ref[64:96, :] = jnp.where(lane32 < 64, rolled, diag[96:])
    own_ref[96:112, :] = jnp.broadcast_to(glob_ref[...], (16, BW)).astype(jnp.bfloat16)


def own_block(owner, q_cols, glob_row):
    return pl.pallas_call(
        own_kernel,
        out_shape=jax.ShapeDtypeStruct((OROWS, BW), jnp.bfloat16),
        grid_spec=pltpu.PrefetchScalarGridSpec(
            num_scalar_prefetch=1,
            grid=(1,),
            in_specs=[
                pl.BlockSpec((BW, BW), lambda i, me: (me[0], 0)),
                pl.BlockSpec((1, BW), lambda i, me: (0, 0)),
            ],
            out_specs=pl.BlockSpec((OROWS, BW), lambda i, me: (0, 0)),
        ),
        cost_estimate=pl.CostEstimate(flops=100_000, bytes_accessed=100_000, transcendentals=0),
        name="own_block",
    )(owner, q_cols, glob_row)


def gmat_kernel(cnt_ref, inv_ref, coup_ref, g_ref, dinv_ref):
    count = cnt_ref[pl.program_id(0)]
    rows, span = coup_ref.shape[1:]
    lane = lax.broadcasted_iota(jnp.int32, (BW, BW), 1)
    row = lax.broadcasted_iota(jnp.int32, (BW, BW), 0)
    mask = (lax.broadcasted_iota(jnp.int32, (1, span), 1) // BW) < count
    for g in range(rows // BW):
        part = slice(g * BW, (g + 1) * BW)
        inv_g = inv_ref[0, part, :]
        full = jnp.dot(inv_g, coup_ref[0, part, :], preferred_element_type=jnp.float32)
        g_ref[0, part, :] = jnp.where(mask, full, 0.0).astype(jnp.bfloat16)
        inv_f = inv_g.astype(jnp.float32)
        dinv_ref[0, g : g + 1, :] = jnp.sum(jnp.where(lane == row, inv_f, 0.0), axis=0, keepdims=True)


def gmat_call(counts, inv_blocks, coupling):
    days, rows, span = coupling.shape
    groups = rows // BW
    return pl.pallas_call(
        gmat_kernel,
        out_shape=(
            jax.ShapeDtypeStruct((days, rows, span), jnp.bfloat16),
            jax.ShapeDtypeStruct((days, groups, BW), jnp.float32),
        ),
        grid_spec=pltpu.PrefetchScalarGridSpec(
            num_scalar_prefetch=1,
            grid=(days,),
            in_specs=[
                pl.BlockSpec((1, rows, BW), lambda i, *_: (i, 0, 0)),
                pl.BlockSpec((1, rows, span), lambda i, *_: (i, 0, 0)),
            ],
            out_specs=[
                pl.BlockSpec((1, rows, span), lambda i, *_: (i, 0, 0)),
                pl.BlockSpec((1, groups, BW), lambda i, *_: (i, 0, 0)),
            ],
        ),
        cost_estimate=pl.CostEstimate(
            flops=8 * days * rows * span * BW, bytes_accessed=days * rows * span * 4, transcendentals=0
        ),
        name="gmat",
    )(counts, inv_blocks, coupling)


def solve_kernel(cnt_ref, inv_ref, coup_ref, rhs_ref, x_ref, sol_ref):
    count = cnt_ref[pl.program_id(0)]
    rows = coup_ref.shape[1]
    groups = rows // BW
    rhs_t = rhs_ref[0].T
    lane = lax.broadcasted_iota(jnp.int32, (BW, BW), 1)
    x_row = [jnp.where(k < count, x_ref[k, 0:1, :].astype(jnp.float32), 0.0) for k in range(KMAX)]
    solved = jnp.zeros((BW, BW), jnp.float32)
    for g in range(groups):
        part = slice(g * BW, (g + 1) * BW)
        acc = coup_ref[0, part, 0:BW].astype(jnp.float32) * x_row[0]
        for k in range(1, KMAX):
            acc += coup_ref[0, part, k * BW : (k + 1) * BW].astype(jnp.float32) * x_row[k]
        dots = jnp.sum(acc, axis=1, keepdims=True)
        resid = rhs_t[:, g : g + 1] - dots
        resid = jnp.where(lane == g, resid, 0.0).astype(jnp.bfloat16)
        solved += jnp.dot(inv_ref[0, part, :], resid, preferred_element_type=jnp.float32)
    sol_ref[0] = solved.T[:groups]


def solve_call(counts, inv_blocks, coupling, rhs, diags):
    days, rows, span = coupling.shape
    groups = rows // BW
    return pl.pallas_call(
        solve_kernel,
        out_shape=jax.ShapeDtypeStruct((days, groups, BW), jnp.float32),
        grid_spec=pltpu.PrefetchScalarGridSpec(
            num_scalar_prefetch=1,
            grid=(days,),
            in_specs=[
                pl.BlockSpec((1, rows, BW), lambda i, *_: (i, 0, 0)),
                pl.BlockSpec((1, rows, span), lambda i, *_: (i, 0, 0)),
                pl.BlockSpec((1, groups, BW), lambda i, *_: (i, 0, 0)),
                pl.BlockSpec((KMAX, 16, BW), lambda i, *_: (i, OROWS // 16 - 1, 0)),
            ],
            out_specs=pl.BlockSpec((1, groups, BW), lambda i, *_: (i, 0, 0)),
        ),
        cost_estimate=pl.CostEstimate(
            flops=4 * days * rows * span * BW, bytes_accessed=days * rows * span * 2, transcendentals=0
        ),
        name="solve",
    )(counts, inv_blocks, coupling, rhs, diags)


def collect_kernel(chunks, st_ref, got_ref, *refs):
    n_out = len(chunks)
    outs = refs[:n_out]
    buf, in_sem, out_sem = refs[n_out:]
    slots = buf.shape[0]

    def copy_in(p):
        return pltpu.make_async_copy(got_ref.at[st_ref[p]], buf.at[p], in_sem.at[p])

    @pl.loop(0, slots)
    def _(p):
        copy_in(p).start()

    made = []
    first = 0
    for n, (days, _) in enumerate(chunks):
        here = slice(first * KMAX, (first + days) * KMAX)

        @pl.loop(first * KMAX, (first + days) * KMAX)
        def _(p):
            copy_in(p).wait()

        copy = pltpu.make_async_copy(buf.at[here], outs[n], out_sem.at[n])
        copy.start()
        made.append(copy)
        first += days
    for copy in made:
        copy.wait()


def collect(my_st, got):
    slots = my_st.shape[0]
    shapes = [(days * KMAX, QROWS, BW) for days, _ in CHUNKS]
    any_spec = pl.BlockSpec(memory_space=pl.ANY)
    return pl.pallas_call(
        functools.partial(collect_kernel, CHUNKS),
        out_shape=tuple(jax.ShapeDtypeStruct(shape, got.dtype) for shape in shapes),
        grid_spec=pltpu.PrefetchScalarGridSpec(
            num_scalar_prefetch=1,
            grid=(1,),
            in_specs=[any_spec],
            out_specs=[any_spec] * len(shapes),
            scratch_shapes=[
                pltpu.VMEM((slots, QROWS, BW), got.dtype),
                pltpu.SemaphoreType.DMA((slots,)),
                pltpu.SemaphoreType.DMA((len(shapes),)),
            ],
        ),
        cost_estimate=pl.CostEstimate(flops=1_000_000, bytes_accessed=4_000_000, transcendentals=0),
        name="collect",
    )(my_st, got)


def diag_pick_kernel(st_ref, all_ref, out_ref, buf, in_sem, out_sem):
    slots = buf.shape[0]

    def copy_in(p):
        return pltpu.make_async_copy(all_ref.at[st_ref[p]], buf.at[p], in_sem.at[p])

    @pl.loop(0, slots)
    def _(p):
        copy_in(p).start()

    @pl.loop(0, slots)
    def _(p):
        copy_in(p).wait()

    copy = pltpu.make_async_copy(buf, out_ref, out_sem.at[0])
    copy.start()
    copy.wait()


def diag_pick(my_st, blocks):
    slots = my_st.shape[0]
    any_spec = pl.BlockSpec(memory_space=pl.ANY)
    return pl.pallas_call(
        diag_pick_kernel,
        out_shape=jax.ShapeDtypeStruct((slots, OROWS, BW), blocks.dtype),
        grid_spec=pltpu.PrefetchScalarGridSpec(
            num_scalar_prefetch=1,
            grid=(1,),
            in_specs=[any_spec],
            out_specs=any_spec,
            scratch_shapes=[
                pltpu.VMEM((slots, OROWS, BW), blocks.dtype),
                pltpu.SemaphoreType.DMA((slots,)),
                pltpu.SemaphoreType.DMA((1,)),
            ],
        ),
        cost_estimate=pl.CostEstimate(flops=1_000_000, bytes_accessed=4_000_000, transcendentals=0),
        name="diag_pick",
    )(my_st, blocks)


def accumulate(g_ref, weights, window, depth, base_ref, out_ref):
    rows = g_ref.shape[1]
    block = 512
    for r in range(rows // block):
        here = slice(r * block, (r + 1) * block)
        acc = jnp.zeros((block, BW), jnp.float32)
        for j in range(KMAX // 2):
            begin = (2 * j + window) % KMAX
            end = min(begin + depth, KMAX)
            left = g_ref[0, here, begin * BW : end * BW]
            if end - begin < depth:
                left = jnp.concatenate([left, g_ref[0, here, : (depth - end + begin) * BW]], axis=1)
            h = jnp.dot(left, weights[j], preferred_element_type=jnp.float32)
            prod = h * g_ref[0, here, j * 2 * BW : (j + 1) * 2 * BW].astype(jnp.float32)
            acc += prod[:, :BW] + prod[:, BW:]
        for b in range(block // BW):
            g = r * (block // BW) + b
            total = jnp.sum(acc[b * BW : (b + 1) * BW].T, axis=0, keepdims=True)
            out_ref[0, g : g + 1, :] = base_ref[0, g : g + 1, :] + 2.0 * total


def diag_kernel(g_ref, base_ref, own_ref, out_ref, weights):
    @pl.when(pl.program_id(0) == 0)
    def _():
        weights[...] = jnp.zeros_like(weights)

    lane64 = lax.broadcasted_iota(jnp.int32, (64, BW), 1)
    for k in range(KMAX):
        j, low = k // 2, (k % 2) * BW
        lanes = slice(low, low + BW)
        top = own_ref[k, 0:64, :].astype(jnp.float32)
        corner = own_ref[k, 64:96, :].astype(jnp.float32)
        bottom = jnp.concatenate([pltpu.roll(corner, 64, 1), corner], axis=0)
        weights[j, low : low + 64, lanes] = jnp.where(lane64 < 64, 0.5 * top, top).astype(jnp.bfloat16)
        weights[j, low + 64 : low + 128, lanes] = jnp.where(lane64 >= 64, 0.5 * bottom, 0.0).astype(jnp.bfloat16)
    accumulate(g_ref, weights, 0, 2, base_ref, out_ref)


def diag_call(gmat, dinv, diags):
    days, rows, span = gmat.shape
    groups = rows // BW
    return pl.pallas_call(
        diag_kernel,
        out_shape=jax.ShapeDtypeStruct((days, groups, BW), jnp.float32),
        grid_spec=pltpu.PrefetchScalarGridSpec(
            num_scalar_prefetch=0,
            grid=(days,),
            in_specs=[
                pl.BlockSpec((1, rows, span), lambda i: (i, 0, 0)),
                pl.BlockSpec((1, groups, BW), lambda i: (i, 0, 0)),
                pl.BlockSpec((KMAX, OROWS, BW), lambda i: (i, 0, 0)),
            ],
            out_specs=pl.BlockSpec((1, groups, BW), lambda i: (i, 0, 0)),
            scratch_shapes=[pltpu.VMEM((KMAX // 2, 2 * BW, 2 * BW), jnp.bfloat16)],
        ),
        cost_estimate=pl.CostEstimate(
            flops=2 * days * rows * span * 2 * BW, bytes_accessed=days * rows * span * 2, transcendentals=0
        ),
        name="diag",
    )(gmat, dinv, diags)


def cov_kernel(lengths, me_ref, g_ref, base_ref, *refs):
    n_in = 4 * len(lengths) + 1
    out_ref, items, weights, sems = refs[n_in:]
    step = pl.program_id(0)
    me = me_ref[0]
    total_days = sum(lengths)
    quad = KMAX // 2

    def copies(chunk, day, slot):
        made = []
        for n, away in enumerate((0, 3, 1, 2)):
            ref = refs[4 * chunk + n]
            made.append(
                pltpu.make_async_copy(
                    ref.at[pl.ds(day * KMAX, KMAX)], items.at[slot, lax.rem(me + away, 4)], sems.at[slot, n]
                )
            )
        return made

    def start(day, slot):
        first = 0
        for chunk, length in enumerate(lengths):

            @pl.when((day >= first) & (day < first + length))
            def _(chunk=chunk, first=first):
                for copy in copies(chunk, day - first, slot):
                    copy.start()

            first += length

    @pl.when(step == 0)
    def _():
        weights[...] = jnp.zeros_like(weights)
        start(step, 0)

    slot = lax.rem(step, 2)
    for copy in copies(0, 0, slot):
        copy.wait()

    @pl.when(step + 1 < total_days)
    def _():
        start(step + 1, 1 - slot)

    lane64 = lax.broadcasted_iota(jnp.int32, (64, BW), 1)
    for k in range(KMAX):
        j, e = k // 2, k % 2
        lanes = slice(e * BW, (e + 1) * BW)
        for n in range(3):
            low = (e + n) * BW
            for q in range(4):
                weights[j, low + 32 * q : low + 32 * (q + 1), lanes] = items[slot, q, k, 32 * n : 32 * (n + 1), :]
        far = jnp.concatenate([items[slot, q, k, 96:112, :] for q in range(4)], axis=0)
        low = (e + 3) * BW
        if k < quad:
            weights[j, low : low + 64, lanes] = far
        else:
            far = far.astype(jnp.float32)
            left = jnp.where(lane64 >= 64, pltpu.roll(far, 64, 1), 0.0)
            weights[j, low : low + 64, lanes] = left.astype(jnp.bfloat16)
            weights[j, low + 64 : low + 128, lanes] = jnp.where(lane64 >= 64, far, 0.0).astype(jnp.bfloat16)
    accumulate(g_ref, weights, 1, 5, base_ref, out_ref)


def cov_call(me, gmat, base, chunks, last, first):
    rows, span = gmat.shape[1:]
    groups = rows // BW
    lengths = tuple(chunk[0] for chunk in chunks)
    days = sum(lengths)
    depth = 5 * BW
    arrays = [array for chunk in chunks for array in chunk[1:]] + [last]
    return pl.pallas_call(
        functools.partial(cov_kernel, lengths),
        out_shape=jax.ShapeDtypeStruct((days, groups, BW), jnp.float32),
        grid_spec=pltpu.PrefetchScalarGridSpec(
            num_scalar_prefetch=1,
            grid=(days,),
            in_specs=[
                pl.BlockSpec((1, rows, span), lambda i, *_: (i + first, 0, 0)),
                pl.BlockSpec((1, groups, BW), lambda i, *_: (i + first, 0, 0)),
            ]
            + [pl.BlockSpec(memory_space=pl.ANY)] * len(arrays),
            out_specs=pl.BlockSpec((1, groups, BW), lambda i, *_: (i, 0, 0)),
            scratch_shapes=[
                pltpu.VMEM((2, 4, KMAX, QROWS, BW), jnp.bfloat16),
                pltpu.VMEM((KMAX // 2, depth, 2 * BW), jnp.bfloat16),
                pltpu.SemaphoreType.DMA((2, 4)),
            ],
        ),
        cost_estimate=pl.CostEstimate(
            flops=2 * days * rows * span * depth, bytes_accessed=days * rows * span * 2, transcendentals=0
        ),
    )(me, gmat, base, *arrays)


def local(stations, counts, q_cols, glob_solution, inv_blocks, coupling, local_rhs):
    shards = lax.axis_size("days")
    ncols = lax.axis_size("cols")
    me = lax.axis_index("cols")
    my_shard = lax.axis_index("days")
    owner = my_shard * ncols + me
    day_dev, rows, _ = inv_blocks.shape
    slots = day_dev * KMAX
    groups = rows // BW

    shard_st = stations.reshape(shards, slots)
    order = jnp.arange(slots, dtype=jnp.int32)
    pos = jnp.max(jnp.where(shard_st == owner, order[None, :], -1), axis=1)
    st_flat = stations.reshape(-1)
    glob_row = glob_solution.reshape(1, BW)
    my_st = lax.dynamic_slice_in_dim(stations, my_shard * day_dev, day_dev, 0).reshape(slots)
    my_counts = lax.dynamic_slice_in_dim(counts, my_shard * day_dev, day_dev, 0)
    rhs = local_rhs.reshape(day_dev, groups, BW)
    perms = {
        "ahead": [(i, (i + 1) % ncols) for i in range(ncols)],
        "back": [(i, (i - 1) % ncols) for i in range(ncols)],
        "direct": [(i, (i + 2) % ncols) for i in range(ncols)],
    }
    me = me.reshape(1)

    own = own_block(owner.reshape(1), q_cols, glob_row)
    own_blocks = lax.all_gather(own, ("days", "cols"), axis=0)
    items = pack_items(pos, st_flat, q_cols, shards, day_dev)
    got = lax.all_to_all(
        items.reshape(shards * ncols, QROWS, BW), ("days", "cols"), split_axis=0, concat_axis=0, tiled=True
    )
    gmat, dinv = gmat_call(my_counts, inv_blocks, coupling)
    owns = collect(my_st, got)
    chunks = []
    for (days, way), own in zip(CHUNKS, owns):
        behind = lax.ppermute(own, "cols", perms["ahead"])
        before = lax.ppermute(own, "cols", perms["back"])
        far = lax.ppermute({"ahead": behind, "back": before, "direct": own}[way], "cols", perms[way])
        chunks.append((days, own, behind, before, far))
    diags = diag_pick(my_st, own_blocks)
    solved = solve_call(my_counts, inv_blocks, coupling, rhs, diags)
    base = diag_call(gmat, dinv, diags)
    early = sum(chunk[0] for chunk in chunks[:2])
    cov_0 = cov_call(me, gmat, base, chunks[:2], base, 0)
    cov_1 = cov_call(me, gmat, base, chunks[2:], cov_0, early)
    cov = jnp.concatenate([cov_0, cov_1], axis=0)
    return solved.reshape(day_dev, rows), cov.reshape(day_dev, rows)


def solution(mesh):
    return jax.shard_map(
        local,
        mesh=mesh,
        in_specs=(
            P(),
            P(),
            P(None, ("days", "cols")),
            P(("days", "cols")),
            P("days", "cols", None),
            P("days", "cols", None),
            P("days", "cols"),
        ),
        out_specs=(P("days", "cols"), P("days", "cols")),
        check_vma=False,
    )
```

```python
import functools

import jax
import jax.numpy as jnp
from jax import lax
from jax.experimental import pallas as pl
from jax.experimental.pallas import tpu as pltpu
from jax.sharding import PartitionSpec as P


BW = 128
KMAX = 8
ROWS = (64, 80)
OFFSETS = ((0, 1), (2, 3, 4))
CHUNKS = (((4, "ahead"), (4, "back")), ((3, "ahead"), (3, "back"), (2, "direct")))


def pack_kernel(part, shards, day_dev, pos_ref, st_ref, q_ref, glob_ref, out_ref, blocks, items, in_sem, out_sem):
    slots = day_dev * KMAX

    def copies(shard):
        pos = pos_ref[shard]
        day = pos // KMAX
        slot = pos % KMAX
        made = []
        for n, off in enumerate(OFFSETS[part]):
            other = st_ref[shard * slots + day * KMAX + (slot + off) % KMAX]
            rows = pl.ds(pl.multiple_of(other * BW, BW), BW)
            made.append(pltpu.make_async_copy(q_ref.at[rows, :], blocks.at[shard, n], in_sem.at[shard, n]))
        return made

    def out_copy(shard):
        return pltpu.make_async_copy(items.at[shard], out_ref.at[shard], out_sem.at[shard])

    @pl.loop(0, shards)
    def _(shard):
        @pl.when(pos_ref[shard] >= 0)
        def _():
            for copy in copies(shard):
                copy.start()

    x_rows = jnp.broadcast_to(glob_ref[...], (8, BW))

    def fill_first(shard):
        diag = blocks[shard, 0]
        lane32 = lax.broadcasted_iota(jnp.int32, (32, BW), 1)
        corner = jnp.where(
            lane32 < 64,
            pltpu.roll(diag[64:96].astype(jnp.float32), 64, 1),
            diag[96:].astype(jnp.float32),
        )
        for q in range(4):
            items[shard, q, 0:32, :] = blocks[shard, 1, 32 * q : 32 * (q + 1), :]
            items[shard, q, 32:48, :] = diag[16 * q : 16 * (q + 1)]
            items[shard, q, 48:64, :] = jnp.concatenate([corner[8 * q : 8 * (q + 1)], x_rows], axis=0).astype(
                jnp.bfloat16
            )

    def fill_second(shard):
        upper = (pos_ref[shard] % KMAX) < KMAX // 2
        half = blocks[shard, 2]
        lane = lax.broadcasted_iota(jnp.int32, (64, BW), 1)
        rolled = pltpu.roll(half[:64].astype(jnp.float32), 64, 1).astype(jnp.bfloat16)
        half = jnp.where(upper, half[:64], jnp.where(lane < 64, rolled, half[64:]))
        for q in range(4):
            for n in range(2):
                items[shard, q, 32 * n : 32 * (n + 1), :] = blocks[shard, n, 32 * q : 32 * (q + 1), :]
            items[shard, q, 64:80, :] = half[16 * q : 16 * (q + 1)]

    @pl.loop(0, shards)
    def _(shard):
        @pl.when(pos_ref[shard] >= 0)
        def _():
            for copy in copies(shard):
                copy.wait()
            (fill_first, fill_second)[part](shard)
            out_copy(shard).start()

    @pl.loop(0, shards)
    def _(shard):
        @pl.when(pos_ref[shard] >= 0)
        def _():
            out_copy(shard).wait()


def pack_items(part, pos, st_flat, q_cols, glob_row, shards, day_dev):
    n_off = len(OFFSETS[part])
    return pl.pallas_call(
        functools.partial(pack_kernel, part, shards, day_dev),
        out_shape=jax.ShapeDtypeStruct((shards, 4, ROWS[part], BW), jnp.bfloat16),
        grid_spec=pltpu.PrefetchScalarGridSpec(
            num_scalar_prefetch=2,
            grid=(1,),
            in_specs=[
                pl.BlockSpec(memory_space=pl.ANY),
                pl.BlockSpec((1, BW), lambda i, *_: (0, 0)),
            ],
            out_specs=pl.BlockSpec(memory_space=pl.ANY),
            scratch_shapes=[
                pltpu.VMEM((shards, n_off, BW, BW), jnp.bfloat16),
                pltpu.VMEM((shards, 4, ROWS[part], BW), jnp.bfloat16),
                pltpu.SemaphoreType.DMA((shards, n_off)),
                pltpu.SemaphoreType.DMA((shards,)),
            ],
        ),
        cost_estimate=pl.CostEstimate(flops=5_000_000, bytes_accessed=5_000_000, transcendentals=0),
    )(pos, st_flat, q_cols, glob_row)


def gmat_kernel(cnt_ref, inv_ref, coup_ref, g_ref, dinv_ref):
    count = cnt_ref[pl.program_id(0)]
    rows, span = coup_ref.shape[1:]
    lane = lax.broadcasted_iota(jnp.int32, (BW, BW), 1)
    row = lax.broadcasted_iota(jnp.int32, (BW, BW), 0)
    mask = (lax.broadcasted_iota(jnp.int32, (1, span), 1) // BW) < count
    for g in range(rows // BW):
        part = slice(g * BW, (g + 1) * BW)
        inv_g = inv_ref[0, part, :]
        full = jnp.dot(inv_g, coup_ref[0, part, :], preferred_element_type=jnp.float32)
        g_ref[0, part, :] = jnp.where(mask, full, 0.0).astype(jnp.bfloat16)
        inv_f = inv_g.astype(jnp.float32)
        dinv_ref[0, g : g + 1, :] = jnp.sum(jnp.where(lane == row, inv_f, 0.0), axis=0, keepdims=True)


def gmat_call(counts, inv_blocks, coupling):
    days, rows, span = coupling.shape
    groups = rows // BW
    return pl.pallas_call(
        gmat_kernel,
        out_shape=(
            jax.ShapeDtypeStruct((days, rows, span), jnp.bfloat16),
            jax.ShapeDtypeStruct((days, groups, BW), jnp.float32),
        ),
        grid_spec=pltpu.PrefetchScalarGridSpec(
            num_scalar_prefetch=1,
            grid=(days,),
            in_specs=[
                pl.BlockSpec((1, rows, BW), lambda i, *_: (i, 0, 0)),
                pl.BlockSpec((1, rows, span), lambda i, *_: (i, 0, 0)),
            ],
            out_specs=[
                pl.BlockSpec((1, rows, span), lambda i, *_: (i, 0, 0)),
                pl.BlockSpec((1, groups, BW), lambda i, *_: (i, 0, 0)),
            ],
        ),
        cost_estimate=pl.CostEstimate(
            flops=8 * days * rows * span * BW, bytes_accessed=days * rows * span * 4, transcendentals=0
        ),
        name="gmat",
    )(counts, inv_blocks, coupling)


def solve_kernel(cnt_ref, inv_ref, coup_ref, rhs_ref, x_ref, sol_ref):
    count = cnt_ref[pl.program_id(0)]
    rows = coup_ref.shape[1]
    groups = rows // BW
    x8 = jnp.concatenate([x_ref[0, k, 8:9, :].astype(jnp.float32) for k in range(KMAX)], axis=0)
    keep = lax.broadcasted_iota(jnp.int32, (KMAX, BW), 0) < count
    x_t = jnp.where(keep, x8, 0.0).T
    rhs_t = rhs_ref[0].T
    x_col = jnp.concatenate(
        [jnp.broadcast_to(x_t[:, k : k + 1], (BW, BW)) for k in range(KMAX)], axis=0
    ).astype(jnp.bfloat16)
    lane = lax.broadcasted_iota(jnp.int32, (BW, BW), 1)
    dots = jnp.dot(coup_ref[0], x_col, preferred_element_type=jnp.float32)
    solved = jnp.zeros((BW, BW), jnp.float32)
    for g in range(groups):
        part = slice(g * BW, (g + 1) * BW)
        resid = (rhs_t[:, g : g + 1] - dots[part]).astype(jnp.bfloat16)
        resid = jnp.where(lane == g, resid, jnp.zeros_like(resid))
        solved += jnp.dot(inv_ref[0, part, :], resid, preferred_element_type=jnp.float32)
    sol_ref[0] = solved.T[:groups]


def solve_call(counts, inv_blocks, coupling, rhs, x_rows):
    days, rows, span = coupling.shape
    groups = rows // BW
    return pl.pallas_call(
        solve_kernel,
        out_shape=jax.ShapeDtypeStruct((days, groups, BW), jnp.float32),
        grid_spec=pltpu.PrefetchScalarGridSpec(
            num_scalar_prefetch=1,
            grid=(days,),
            in_specs=[
                pl.BlockSpec((1, rows, BW), lambda i, *_: (i, 0, 0)),
                pl.BlockSpec((1, rows, span), lambda i, *_: (i, 0, 0)),
                pl.BlockSpec((1, groups, BW), lambda i, *_: (i, 0, 0)),
                pl.BlockSpec((1, KMAX, 16, BW), lambda i, *_: (i, 0, 0, 0)),
            ],
            out_specs=pl.BlockSpec((1, groups, BW), lambda i, *_: (i, 0, 0)),
        ),
        cost_estimate=pl.CostEstimate(
            flops=4 * days * rows * span * BW, bytes_accessed=days * rows * span * 2, transcendentals=0
        ),
        name="solve",
    )(counts, inv_blocks, coupling, rhs, x_rows)


def collect_kernel(part, chunks, st_ref, got_ref, *refs):
    n_out = len(chunks) + (part == 0)
    outs = refs[:n_out]
    buf, in_sem, out_sem = refs[n_out:]
    slots = buf.shape[0]

    def copy_in(p):
        return pltpu.make_async_copy(got_ref.at[st_ref[p]], buf.at[p], in_sem.at[p])

    @pl.loop(0, slots)
    def _(p):
        copy_in(p).start()

    made = []
    first = 0
    for n, (days, _) in enumerate(chunks):
        here = slice(first * KMAX, (first + days) * KMAX)

        @pl.loop(first * KMAX, (first + days) * KMAX)
        def _(p):
            copy_in(p).wait()

        copy = pltpu.make_async_copy(buf.at[here], outs[n], out_sem.at[n])
        copy.start()
        made.append(copy)
        first += days
    if part == 0:
        copy = pltpu.make_async_copy(buf.at[:, ROWS[0] - 16 :, :], outs[-1], out_sem.at[len(chunks)])
        copy.start()
        made.append(copy)
    for copy in made:
        copy.wait()


def collect(part, my_st, got):
    slots = my_st.shape[0]
    chunks = CHUNKS[part]
    shapes = [(days * KMAX, ROWS[part], BW) for days, _ in chunks]
    if part == 0:
        shapes.append((slots, 16, BW))
    any_spec = pl.BlockSpec(memory_space=pl.ANY)
    return pl.pallas_call(
        functools.partial(collect_kernel, part, chunks),
        out_shape=tuple(jax.ShapeDtypeStruct(shape, got.dtype) for shape in shapes),
        grid_spec=pltpu.PrefetchScalarGridSpec(
            num_scalar_prefetch=1,
            grid=(1,),
            in_specs=[any_spec],
            out_specs=[any_spec] * len(shapes),
            scratch_shapes=[
                pltpu.VMEM((slots, ROWS[part], BW), got.dtype),
                pltpu.SemaphoreType.DMA((slots,)),
                pltpu.SemaphoreType.DMA((len(shapes),)),
            ],
        ),
        cost_estimate=pl.CostEstimate(flops=1_000_000, bytes_accessed=2_500_000, transcendentals=0),
    )(my_st, got)


def cov_kernel(part, lengths, me_ref, g_ref, base_ref, *refs):
    n_in = 4 * len(lengths) + 1
    out_ref, items, weights, sems = refs[n_in:]
    step = pl.program_id(0)
    me = me_ref[0]
    total_days = sum(lengths)
    rows, _ = g_ref.shape[1:]
    quad = KMAX // 2
    window = OFFSETS[part][0]
    depth = OFFSETS[part][-1] + 2 - window

    def copies(chunk, day, slot):
        made = []
        for n, away in enumerate((0, 3, 1, 2)):
            ref = refs[4 * chunk + n]
            made.append(
                pltpu.make_async_copy(
                    ref.at[pl.ds(day * KMAX, KMAX)], items.at[slot, lax.rem(me + away, 4)], sems.at[slot, n]
                )
            )
        return made

    def start(day, slot):
        first = 0
        for chunk, length in enumerate(lengths):

            @pl.when((day >= first) & (day < first + length))
            def _(chunk=chunk, first=first):
                for copy in copies(chunk, day - first, slot):
                    copy.start()

            first += length

    @pl.when(step == 0)
    def _():
        weights[...] = jnp.zeros_like(weights)
        start(step, 0)

    slot = lax.rem(step, 2)
    for copy in copies(0, 0, slot):
        copy.wait()

    @pl.when(step + 1 < total_days)
    def _():
        start(step + 1, 1 - slot)

    lane64 = lax.broadcasted_iota(jnp.int32, (64, BW), 1)
    for k in range(KMAX):
        j, e = k // 2, k % 2
        lanes = slice(e * BW, (e + 1) * BW)
        for at, off in ((0, 1),) if part == 0 else ((0, 2), (32, 3)):
            low = (e + off - window) * BW
            for q in range(4):
                weights[j, low + 32 * q : low + 32 * (q + 1), lanes] = items[slot, q, k, at : at + 32, :]
        if part == 0:
            top = jnp.concatenate([items[slot, q, k, 32:48, :] for q in range(4)], axis=0).astype(jnp.float32)
            corner = jnp.concatenate([items[slot, q, k, 48:64, :].astype(jnp.float32)[:8] for q in range(4)], axis=0)
            low = e * BW
            weights[j, low : low + 64, lanes] = jnp.where(lane64 < 64, 0.5 * top, top).astype(jnp.bfloat16)
            bottom = jnp.concatenate([pltpu.roll(corner, 64, 1), corner], axis=0)
            weights[j, low + 64 : low + 128, lanes] = jnp.where(lane64 >= 64, 0.5 * bottom, 0.0).astype(jnp.bfloat16)
        else:
            far = jnp.concatenate([items[slot, q, k, 64:80, :] for q in range(4)], axis=0)
            low = (e + 4 - window) * BW
            if k < quad:
                weights[j, low : low + 64, lanes] = far
            else:
                far = far.astype(jnp.float32)
                left = jnp.where(lane64 >= 64, pltpu.roll(far, 64, 1), 0.0)
                weights[j, low : low + 64, lanes] = left.astype(jnp.bfloat16)
                weights[j, low + 64 : low + 128, lanes] = jnp.where(lane64 >= 64, far, 0.0).astype(jnp.bfloat16)

    block = 256
    for r in range(rows // block):
        here = slice(r * block, (r + 1) * block)
        acc = jnp.zeros((block, BW), jnp.float32)
        for j in range(quad):
            begin = (2 * j + window) % KMAX
            end = min(begin + depth, KMAX)
            left = g_ref[0, here, begin * BW : end * BW]
            if end - begin < depth:
                left = jnp.concatenate([left, g_ref[0, here, : (depth - end + begin) * BW]], axis=1)
            h = jnp.dot(left, weights[j], preferred_element_type=jnp.float32)
            prod = h * g_ref[0, here, j * 2 * BW : (j + 1) * 2 * BW].astype(jnp.float32)
            acc += prod[:, :BW] + prod[:, BW:]
        for b in range(block // BW):
            g = r * (block // BW) + b
            total = jnp.sum(acc[b * BW : (b + 1) * BW].T, axis=0, keepdims=True)
            out_ref[0, g : g + 1, :] = base_ref[0, g : g + 1, :] + 2.0 * total


def cov_call(part, me, gmat, base, chunks, last, first, base_first):
    rows, span = gmat.shape[1:]
    groups = rows // BW
    lengths = tuple(chunk[0] for chunk in chunks)
    days = sum(lengths)
    depth = (OFFSETS[part][-1] + 2 - OFFSETS[part][0]) * BW
    arrays = [array for chunk in chunks for array in chunk[1:]] + [last]
    return pl.pallas_call(
        functools.partial(cov_kernel, part, lengths),
        out_shape=jax.ShapeDtypeStruct((days, groups, BW), jnp.float32),
        grid_spec=pltpu.PrefetchScalarGridSpec(
            num_scalar_prefetch=1,
            grid=(days,),
            in_specs=[
                pl.BlockSpec((1, rows, span), lambda i, *_: (i + first, 0, 0)),
                pl.BlockSpec((1, groups, BW), lambda i, *_: (i + base_first, 0, 0)),
            ]
            + [pl.BlockSpec(memory_space=pl.ANY)] * len(arrays),
            out_specs=pl.BlockSpec((1, groups, BW), lambda i, *_: (i, 0, 0)),
            scratch_shapes=[
                pltpu.VMEM((2, 4, KMAX, ROWS[part], BW), jnp.bfloat16),
                pltpu.VMEM((KMAX // 2, depth, 2 * BW), jnp.bfloat16),
                pltpu.SemaphoreType.DMA((2, 4)),
            ],
        ),
        cost_estimate=pl.CostEstimate(
            flops=2 * days * rows * span * depth, bytes_accessed=days * rows * span * 2, transcendentals=0
        ),
    )(me, gmat, base, *arrays)


def local(stations, counts, q_cols, glob_solution, inv_blocks, coupling, local_rhs):
    shards = lax.axis_size("days")
    ncols = lax.axis_size("cols")
    me = lax.axis_index("cols")
    my_shard = lax.axis_index("days")
    owner = my_shard * ncols + me
    day_dev, rows, _ = inv_blocks.shape
    slots = day_dev * KMAX
    groups = rows // BW

    shard_st = stations.reshape(shards, slots)
    order = jnp.arange(slots, dtype=jnp.int32)
    pos = jnp.max(jnp.where(shard_st == owner, order[None, :], -1), axis=1)
    st_flat = stations.reshape(-1)
    glob_row = glob_solution.reshape(1, BW)
    my_st = lax.dynamic_slice_in_dim(stations, my_shard * day_dev, day_dev, 0).reshape(slots)
    my_counts = lax.dynamic_slice_in_dim(counts, my_shard * day_dev, day_dev, 0)
    rhs = local_rhs.reshape(day_dev, groups, BW)
    me = me.reshape(1)
    perms = {
        "ahead": [(i, (i + 1) % ncols) for i in range(ncols)],
        "back": [(i, (i - 1) % ncols) for i in range(ncols)],
        "direct": [(i, (i + 2) % ncols) for i in range(ncols)],
    }

    def exchange(part):
        items = pack_items(part, pos, st_flat, q_cols, glob_row, shards, day_dev)
        return lax.all_to_all(
            items.reshape(shards * ncols, ROWS[part], BW),
            ("days", "cols"),
            split_axis=0,
            concat_axis=0,
            tiled=True,
        )

    def ring(part, owns):
        chunks = []
        for (days, way), own in zip(CHUNKS[part], owns):
            behind = lax.ppermute(own, "cols", perms["ahead"])
            before = lax.ppermute(own, "cols", perms["back"])
            far = lax.ppermute({"ahead": behind, "back": before, "direct": own}[way], "cols", perms[way])
            chunks.append((days, own, behind, before, far))
        return chunks

    got_a, got_b = exchange(0), exchange(1)
    gmat, dinv = gmat_call(my_counts, inv_blocks, coupling)
    *owns_a, x_rows = collect(0, my_st, got_a)
    chunks_a = ring(0, owns_a)
    solved = solve_call(my_counts, inv_blocks, coupling, rhs, x_rows.reshape(day_dev, KMAX, 16, BW))
    owns_b = collect(1, my_st, got_b)
    chunks_b = ring(1, owns_b)
    half = cov_call(0, me, gmat, dinv, chunks_a, dinv, 0, 0)
    early = sum(chunk[0] for chunk in chunks_b[:2])
    cov_0 = cov_call(1, me, gmat, half, chunks_b[:2], half, 0, 0)
    cov_1 = cov_call(1, me, gmat, half, chunks_b[2:], cov_0, early, early)
    cov = jnp.concatenate([cov_0, cov_1], axis=0)
    return solved.reshape(day_dev, rows), cov.reshape(day_dev, rows)


def solution(mesh):
    return jax.shard_map(
        local,
        mesh=mesh,
        in_specs=(
            P(),
            P(),
            P(None, ("days", "cols")),
            P(("days", "cols")),
            P("days", "cols", None),
            P("days", "cols", None),
            P("days", "cols"),
        ),
        out_specs=(P("days", "cols"), P("days", "cols")),
        check_vma=False,
    )
```

```python
import functools

import jax
import jax.numpy as jnp
from jax import lax
from jax.experimental import pallas as pl
from jax.experimental.pallas import tpu as pltpu
from jax.sharding import PartitionSpec as P


BW = 128
KMAX = 8
ROWS = (64, 80)
OFFSETS = ((0, 1), (2, 3, 4))
CHUNKS = (((4, "ahead"), (4, "back")), ((3, "ahead"), (3, "back"), (2, "direct")))


def pack_kernel(part, shards, day_dev, pos_ref, st_ref, q_ref, glob_ref, out_ref, blocks, items, in_sem, out_sem):
    slots = day_dev * KMAX

    def copies(shard):
        pos = pos_ref[shard]
        day = pos // KMAX
        slot = pos % KMAX
        made = []
        for n, off in enumerate(OFFSETS[part]):
            other = st_ref[shard * slots + day * KMAX + (slot + off) % KMAX]
            rows = pl.ds(pl.multiple_of(other * BW, BW), BW)
            made.append(pltpu.make_async_copy(q_ref.at[rows, :], blocks.at[shard, n], in_sem.at[shard, n]))
        return made

    def out_copy(shard):
        return pltpu.make_async_copy(items.at[shard], out_ref.at[shard], out_sem.at[shard])

    @pl.loop(0, shards)
    def _(shard):
        @pl.when(pos_ref[shard] >= 0)
        def _():
            for copy in copies(shard):
                copy.start()

    x_rows = jnp.broadcast_to(glob_ref[...], (8, BW))

    def fill_first(shard):
        diag = blocks[shard, 0]
        lane32 = lax.broadcasted_iota(jnp.int32, (32, BW), 1)
        corner = jnp.where(
            lane32 < 64,
            pltpu.roll(diag[64:96].astype(jnp.float32), 64, 1),
            diag[96:].astype(jnp.float32),
        )
        for q in range(4):
            items[shard, q, 0:32, :] = blocks[shard, 1, 32 * q : 32 * (q + 1), :]
            items[shard, q, 32:48, :] = diag[16 * q : 16 * (q + 1)]
            items[shard, q, 48:64, :] = jnp.concatenate([corner[8 * q : 8 * (q + 1)], x_rows], axis=0).astype(
                jnp.bfloat16
            )

    def fill_second(shard):
        upper = (pos_ref[shard] % KMAX) < KMAX // 2
        half = blocks[shard, 2]
        lane = lax.broadcasted_iota(jnp.int32, (64, BW), 1)
        rolled = pltpu.roll(half[:64].astype(jnp.float32), 64, 1).astype(jnp.bfloat16)
        half = jnp.where(upper, half[:64], jnp.where(lane < 64, rolled, half[64:]))
        for q in range(4):
            for n in range(2):
                items[shard, q, 32 * n : 32 * (n + 1), :] = blocks[shard, n, 32 * q : 32 * (q + 1), :]
            items[shard, q, 64:80, :] = half[16 * q : 16 * (q + 1)]

    @pl.loop(0, shards)
    def _(shard):
        @pl.when(pos_ref[shard] >= 0)
        def _():
            for copy in copies(shard):
                copy.wait()
            (fill_first, fill_second)[part](shard)
            out_copy(shard).start()

    @pl.loop(0, shards)
    def _(shard):
        @pl.when(pos_ref[shard] >= 0)
        def _():
            out_copy(shard).wait()


def pack_items(part, pos, st_flat, q_cols, glob_row, shards, day_dev):
    n_off = len(OFFSETS[part])
    return pl.pallas_call(
        functools.partial(pack_kernel, part, shards, day_dev),
        out_shape=jax.ShapeDtypeStruct((shards, 4, ROWS[part], BW), jnp.bfloat16),
        grid_spec=pltpu.PrefetchScalarGridSpec(
            num_scalar_prefetch=2,
            grid=(1,),
            in_specs=[
                pl.BlockSpec(memory_space=pl.ANY),
                pl.BlockSpec((1, BW), lambda i, *_: (0, 0)),
            ],
            out_specs=pl.BlockSpec(memory_space=pl.ANY),
            scratch_shapes=[
                pltpu.VMEM((shards, n_off, BW, BW), jnp.bfloat16),
                pltpu.VMEM((shards, 4, ROWS[part], BW), jnp.bfloat16),
                pltpu.SemaphoreType.DMA((shards, n_off)),
                pltpu.SemaphoreType.DMA((shards,)),
            ],
        ),
        cost_estimate=pl.CostEstimate(flops=5_000_000, bytes_accessed=5_000_000, transcendentals=0),
    )(pos, st_flat, q_cols, glob_row)


def gmat_kernel(cnt_ref, inv_ref, coup_ref, g_ref, dinv_ref):
    count = cnt_ref[pl.program_id(0)]
    rows, span = coup_ref.shape[1:]
    lane = lax.broadcasted_iota(jnp.int32, (BW, BW), 1)
    row = lax.broadcasted_iota(jnp.int32, (BW, BW), 0)
    mask = (lax.broadcasted_iota(jnp.int32, (1, span), 1) // BW) < count
    for g in range(rows // BW):
        part = slice(g * BW, (g + 1) * BW)
        inv_g = inv_ref[0, part, :]
        full = jnp.dot(inv_g, coup_ref[0, part, :], preferred_element_type=jnp.float32)
        g_ref[0, part, :] = jnp.where(mask, full, 0.0).astype(jnp.bfloat16)
        inv_f = inv_g.astype(jnp.float32)
        dinv_ref[0, g : g + 1, :] = jnp.sum(jnp.where(lane == row, inv_f, 0.0), axis=0, keepdims=True)


def gmat_call(counts, inv_blocks, coupling):
    days, rows, span = coupling.shape
    groups = rows // BW
    return pl.pallas_call(
        gmat_kernel,
        out_shape=(
            jax.ShapeDtypeStruct((days, rows, span), jnp.bfloat16),
            jax.ShapeDtypeStruct((days, groups, BW), jnp.float32),
        ),
        grid_spec=pltpu.PrefetchScalarGridSpec(
            num_scalar_prefetch=1,
            grid=(days,),
            in_specs=[
                pl.BlockSpec((1, rows, BW), lambda i, *_: (i, 0, 0)),
                pl.BlockSpec((1, rows, span), lambda i, *_: (i, 0, 0)),
            ],
            out_specs=[
                pl.BlockSpec((1, rows, span), lambda i, *_: (i, 0, 0)),
                pl.BlockSpec((1, groups, BW), lambda i, *_: (i, 0, 0)),
            ],
        ),
        cost_estimate=pl.CostEstimate(
            flops=8 * days * rows * span * BW, bytes_accessed=days * rows * span * 4, transcendentals=0
        ),
        name="gmat",
    )(counts, inv_blocks, coupling)


def solve_kernel(cnt_ref, inv_ref, coup_ref, rhs_ref, x_ref, sol_ref):
    count = cnt_ref[pl.program_id(0)]
    rows = coup_ref.shape[1]
    groups = rows // BW
    x8 = jnp.concatenate([x_ref[0, k, 8:9, :].astype(jnp.float32) for k in range(KMAX)], axis=0)
    keep = lax.broadcasted_iota(jnp.int32, (KMAX, BW), 0) < count
    x_t = jnp.where(keep, x8, 0.0).T
    rhs_t = rhs_ref[0].T
    x_col = jnp.concatenate(
        [jnp.broadcast_to(x_t[:, k : k + 1], (BW, BW)) for k in range(KMAX)], axis=0
    ).astype(jnp.bfloat16)
    lane = lax.broadcasted_iota(jnp.int32, (BW, BW), 1)
    dots = jnp.dot(coup_ref[0], x_col, preferred_element_type=jnp.float32)
    solved = jnp.zeros((BW, BW), jnp.float32)
    for g in range(groups):
        part = slice(g * BW, (g + 1) * BW)
        resid = (rhs_t[:, g : g + 1] - dots[part]).astype(jnp.bfloat16)
        resid = jnp.where(lane == g, resid, jnp.zeros_like(resid))
        solved += jnp.dot(inv_ref[0, part, :], resid, preferred_element_type=jnp.float32)
    sol_ref[0] = solved.T[:groups]


def solve_call(counts, inv_blocks, coupling, rhs, x_rows):
    days, rows, span = coupling.shape
    groups = rows // BW
    return pl.pallas_call(
        solve_kernel,
        out_shape=jax.ShapeDtypeStruct((days, groups, BW), jnp.float32),
        grid_spec=pltpu.PrefetchScalarGridSpec(
            num_scalar_prefetch=1,
            grid=(days,),
            in_specs=[
                pl.BlockSpec((1, rows, BW), lambda i, *_: (i, 0, 0)),
                pl.BlockSpec((1, rows, span), lambda i, *_: (i, 0, 0)),
                pl.BlockSpec((1, groups, BW), lambda i, *_: (i, 0, 0)),
                pl.BlockSpec((1, KMAX, 16, BW), lambda i, *_: (i, 0, 0, 0)),
            ],
            out_specs=pl.BlockSpec((1, groups, BW), lambda i, *_: (i, 0, 0)),
        ),
        cost_estimate=pl.CostEstimate(
            flops=4 * days * rows * span * BW, bytes_accessed=days * rows * span * 2, transcendentals=0
        ),
        name="solve",
    )(counts, inv_blocks, coupling, rhs, x_rows)


def collect_kernel(part, chunks, st_ref, got_ref, *outs):
    first = 0
    for n, (days, _) in enumerate(chunks):

        @pl.loop(0, days * KMAX)
        def _(p, n=n, first=first):
            source = st_ref[first + p]
            outs[n][p] = got_ref[source]
            if part == 0:
                outs[-1][first + p] = got_ref[source, ROWS[0] - 16 :, :]

        first += days * KMAX


def collect(part, my_st, got):
    slots = my_st.shape[0]
    chunks = CHUNKS[part]
    shapes = [(days * KMAX, ROWS[part], BW) for days, _ in chunks]
    if part == 0:
        shapes.append((slots, 16, BW))
    vmem_spec = pl.BlockSpec(memory_space=pltpu.VMEM)
    return pl.pallas_call(
        functools.partial(collect_kernel, part, chunks),
        out_shape=tuple(jax.ShapeDtypeStruct(shape, got.dtype) for shape in shapes),
        grid_spec=pltpu.PrefetchScalarGridSpec(
            num_scalar_prefetch=1,
            grid=(1,),
            in_specs=[vmem_spec],
            out_specs=[vmem_spec] * len(shapes),
        ),
        compiler_params=pltpu.CompilerParams(vmem_limit_bytes=16 << 20),
        cost_estimate=pl.CostEstimate(flops=1_000_000, bytes_accessed=2_500_000, transcendentals=0),
    )(my_st, got)


def cov_kernel(part, lengths, me_ref, g_ref, base_ref, *refs):
    n_in = 4 * len(lengths) + 1
    out_ref, items, weights, sems = refs[n_in:]
    step = pl.program_id(0)
    me = me_ref[0]
    total_days = sum(lengths)
    rows, _ = g_ref.shape[1:]
    quad = KMAX // 2
    window = OFFSETS[part][0]
    depth = OFFSETS[part][-1] + 2 - window

    def copies(chunk, day, slot):
        made = []
        for n, away in enumerate((0, 3, 1, 2)):
            ref = refs[4 * chunk + n]
            made.append(
                pltpu.make_async_copy(
                    ref.at[pl.ds(day * KMAX, KMAX)], items.at[slot, lax.rem(me + away, 4)], sems.at[slot, n]
                )
            )
        return made

    def start(day, slot):
        first = 0
        for chunk, length in enumerate(lengths):

            @pl.when((day >= first) & (day < first + length))
            def _(chunk=chunk, first=first):
                for copy in copies(chunk, day - first, slot):
                    copy.start()

            first += length

    @pl.when(step == 0)
    def _():
        weights[...] = jnp.zeros_like(weights)
        start(step, 0)

    slot = lax.rem(step, 2)
    for copy in copies(0, 0, slot):
        copy.wait()

    @pl.when(step + 1 < total_days)
    def _():
        start(step + 1, 1 - slot)

    lane64 = lax.broadcasted_iota(jnp.int32, (64, BW), 1)
    for k in range(KMAX):
        j, e = k // 2, k % 2
        lanes = slice(e * BW, (e + 1) * BW)
        for at, off in ((0, 1),) if part == 0 else ((0, 2), (32, 3)):
            low = (e + off - window) * BW
            for q in range(4):
                weights[j, low + 32 * q : low + 32 * (q + 1), lanes] = items[slot, q, k, at : at + 32, :]
        if part == 0:
            top = jnp.concatenate([items[slot, q, k, 32:48, :] for q in range(4)], axis=0).astype(jnp.float32)
            corner = jnp.concatenate([items[slot, q, k, 48:64, :].astype(jnp.float32)[:8] for q in range(4)], axis=0)
            low = e * BW
            weights[j, low : low + 64, lanes] = jnp.where(lane64 < 64, 0.5 * top, top).astype(jnp.bfloat16)
            bottom = jnp.concatenate([pltpu.roll(corner, 64, 1), corner], axis=0)
            weights[j, low + 64 : low + 128, lanes] = jnp.where(lane64 >= 64, 0.5 * bottom, 0.0).astype(jnp.bfloat16)
        else:
            far = jnp.concatenate([items[slot, q, k, 64:80, :] for q in range(4)], axis=0)
            low = (e + 4 - window) * BW
            if k < quad:
                weights[j, low : low + 64, lanes] = far
            else:
                far = far.astype(jnp.float32)
                left = jnp.where(lane64 >= 64, pltpu.roll(far, 64, 1), 0.0)
                weights[j, low : low + 64, lanes] = left.astype(jnp.bfloat16)
                weights[j, low + 64 : low + 128, lanes] = jnp.where(lane64 >= 64, far, 0.0).astype(jnp.bfloat16)

    block = 256
    for r in range(rows // block):
        here = slice(r * block, (r + 1) * block)
        acc = jnp.zeros((block, BW), jnp.float32)
        for j in range(quad):
            begin = (2 * j + window) % KMAX
            end = min(begin + depth, KMAX)
            left = g_ref[0, here, begin * BW : end * BW]
            if end - begin < depth:
                left = jnp.concatenate([left, g_ref[0, here, : (depth - end + begin) * BW]], axis=1)
            h = jnp.dot(left, weights[j], preferred_element_type=jnp.float32)
            prod = h * g_ref[0, here, j * 2 * BW : (j + 1) * 2 * BW].astype(jnp.float32)
            acc += prod[:, :BW] + prod[:, BW:]
        for b in range(block // BW):
            g = r * (block // BW) + b
            total = jnp.sum(acc[b * BW : (b + 1) * BW].T, axis=0, keepdims=True)
            out_ref[0, g : g + 1, :] = base_ref[0, g : g + 1, :] + 2.0 * total


def cov_call(part, me, gmat, base, chunks, last, first, base_first):
    rows, span = gmat.shape[1:]
    groups = rows // BW
    lengths = tuple(chunk[0] for chunk in chunks)
    days = sum(lengths)
    depth = (OFFSETS[part][-1] + 2 - OFFSETS[part][0]) * BW
    arrays = [array for chunk in chunks for array in chunk[1:]] + [last]
    return pl.pallas_call(
        functools.partial(cov_kernel, part, lengths),
        out_shape=jax.ShapeDtypeStruct((days, groups, BW), jnp.float32),
        grid_spec=pltpu.PrefetchScalarGridSpec(
            num_scalar_prefetch=1,
            grid=(days,),
            in_specs=[
                pl.BlockSpec((1, rows, span), lambda i, *_: (i + first, 0, 0)),
                pl.BlockSpec((1, groups, BW), lambda i, *_: (i + base_first, 0, 0)),
            ]
            + [pl.BlockSpec(memory_space=pl.ANY)] * len(arrays),
            out_specs=pl.BlockSpec((1, groups, BW), lambda i, *_: (i, 0, 0)),
            scratch_shapes=[
                pltpu.VMEM((2, 4, KMAX, ROWS[part], BW), jnp.bfloat16),
                pltpu.VMEM((KMAX // 2, depth, 2 * BW), jnp.bfloat16),
                pltpu.SemaphoreType.DMA((2, 4)),
            ],
        ),
        cost_estimate=pl.CostEstimate(
            flops=2 * days * rows * span * depth, bytes_accessed=days * rows * span * 2, transcendentals=0
        ),
    )(me, gmat, base, *arrays)


def local(stations, counts, q_cols, glob_solution, inv_blocks, coupling, local_rhs):
    shards = lax.axis_size("days")
    ncols = lax.axis_size("cols")
    me = lax.axis_index("cols")
    my_shard = lax.axis_index("days")
    owner = my_shard * ncols + me
    day_dev, rows, _ = inv_blocks.shape
    slots = day_dev * KMAX
    groups = rows // BW

    shard_st = stations.reshape(shards, slots)
    order = jnp.arange(slots, dtype=jnp.int32)
    pos = jnp.max(jnp.where(shard_st == owner, order[None, :], -1), axis=1)
    st_flat = stations.reshape(-1)
    glob_row = glob_solution.reshape(1, BW)
    my_st = lax.dynamic_slice_in_dim(stations, my_shard * day_dev, day_dev, 0).reshape(slots)
    my_counts = lax.dynamic_slice_in_dim(counts, my_shard * day_dev, day_dev, 0)
    rhs = local_rhs.reshape(day_dev, groups, BW)
    me = me.reshape(1)
    perms = {
        "ahead": [(i, (i + 1) % ncols) for i in range(ncols)],
        "back": [(i, (i - 1) % ncols) for i in range(ncols)],
        "direct": [(i, (i + 2) % ncols) for i in range(ncols)],
    }

    def exchange(part):
        items = pack_items(part, pos, st_flat, q_cols, glob_row, shards, day_dev)
        return lax.all_to_all(
            items.reshape(shards * ncols, ROWS[part], BW),
            ("days", "cols"),
            split_axis=0,
            concat_axis=0,
            tiled=True,
        )

    def ring(part, owns):
        chunks = []
        for (days, way), own in zip(CHUNKS[part], owns):
            behind = lax.ppermute(own, "cols", perms["ahead"])
            before = lax.ppermute(own, "cols", perms["back"])
            far = lax.ppermute({"ahead": behind, "back": before, "direct": own}[way], "cols", perms[way])
            chunks.append((days, own, behind, before, far))
        return chunks

    got_a, got_b = exchange(0), exchange(1)
    gmat, dinv = gmat_call(my_counts, inv_blocks, coupling)
    *owns_a, x_rows = collect(0, my_st, got_a)
    chunks_a = ring(0, owns_a)
    solved = solve_call(my_counts, inv_blocks, coupling, rhs, x_rows.reshape(day_dev, KMAX, 16, BW))
    owns_b = collect(1, my_st, got_b)
    chunks_b = ring(1, owns_b)
    half = cov_call(0, me, gmat, dinv, chunks_a, dinv, 0, 0)
    early = sum(chunk[0] for chunk in chunks_b[:2])
    cov_0 = cov_call(1, me, gmat, half, chunks_b[:2], half, 0, 0)
    cov_1 = cov_call(1, me, gmat, half, chunks_b[2:], cov_0, early, early)
    cov = jnp.concatenate([cov_0, cov_1], axis=0)
    return solved.reshape(day_dev, rows), cov.reshape(day_dev, rows)


def solution(mesh):
    return jax.shard_map(
        local,
        mesh=mesh,
        in_specs=(
            P(),
            P(),
            P(None, ("days", "cols")),
            P(("days", "cols")),
            P("days", "cols", None),
            P("days", "cols", None),
            P("days", "cols"),
        ),
        out_specs=(P("days", "cols"), P("days", "cols")),
        check_vma=False,
    )
```
